256 devices in a mesh: site: 2 (over y_lo), rows: 16 (over z, core), width: 8 (over y_hi, x).
Axes of the slice: x: 4, y: 4 (y_hi: 2, y_lo: 2; y = y_hi * 2 + y_lo), z: 8, core: 2. Of those that a mesh axis runs over, the one named last changes fastest.
Arguments:
- one_query: float32 [14336, 7168], P(('site', 'rows'), 'width'), parts along dimension 0, may hold values from -0.09375 to 0.09375
- other_query: float32 [14336, 7168], P(('site', 'rows'), 'width'), parts along dimension 0, may hold values from -0.0625 to 0.0625
- one_key: float32 [14336, 1024], P(('site', 'rows'), 'width'), parts along dimension 0, may hold values from -0.09375 to 0.09375
- other_key: float32 [14336, 1024], P(('site', 'rows'), 'width'), parts along dimension 0, may hold values from -0.0625 to 0.0625
- one_value: float32 [14336, 1024], P(('site', 'rows'), 'width'), parts along dimension 0, may hold values from -0.09375 to 0.09375
- other_value: float32 [14336, 1024], P(('site', 'rows'), 'width'), parts along dimension 0, may hold values from -0.0625 to 0.0625
- mix_share: float32 [14336], P(('site', 'rows')), parts along dimension 0, may hold values from 0.2 to 0.8
- norm_train: float32 [14336], P(('site', 'rows', 'width')), parts along dimension 0, may hold values from 0.25 to 1.75
- norm_step: float32 [14336], P(('site', 'rows', 'width')), parts along dimension 0, may hold values from -0.3 to 0.3
Outputs:
- serving_query: bfloat16 [14336, 7168], P('site', 'width'), parts along dimension 0
- serving_key: bfloat16 [14336, 1024], P('site', 'width'), parts along dimension 0
- serving_value: bfloat16 [14336, 1024], P('site', 'width'), parts along dimension 0
- scale_query: float32 [14336], P(('site', 'width')), parts along dimension 0
- scale_key: float32 [2048], P(('site', 'width')), parts along dimension 0
- scale_value: float32 [2048], P(('site', 'width')), parts along dimension 0
- serve_norm: bfloat16 [14336], P('site'), parts along dimension 0
The draws below stay inside these ranges and needn't reach their ends.
There are 2 independent parts, one for each index of `site`. The reference program is written for one: setup_inputs(seed, part) draws one part's arguments, and reference() takes and returns one part's arrays. A program takes and returns all parts, laid end to end along the dimension named above; each array names one. Nothing has to cross between parts.
All inputs are finite; a program needn't handle non-finite values. Where the reference program divides by a largest or mean magnitude, that divisor is 1e-20 or more.
Results may differ from the reference program's by a relative error of at most 0.001.
Values may be sent and summed in bfloat16 or wider, within the bound.
No kernel may reach another device: no remote copies, remote signals or barrier semaphores. Data moves between devices by JAX's collectives and lax.ppermute only.
A program may use at most 128 MiB of HBM per device.

```python
import jax
import jax.numpy as jnp

D_MODEL = 7168
Q_DIM = 7168
KV_DIM = 1024


def raised(drawn, rng, source, target, blocks, factor):
    def block_of(dim):
        return (jnp.arange(drawn.shape[dim]) // (drawn.shape[dim] // blocks)).reshape((-1,) + (1,) * (drawn.ndim - 1 - dim))

    first = jax.random.permutation(rng, blocks)[block_of(target)]
    other_side = (block_of(target) + blocks // 2) % blocks
    return jnp.where((block_of(source) == first) | (block_of(source) == other_side), factor * drawn, drawn)


def level_of(own_key, dims, cuts, least, largest):
    loudness = 1.0
    for position, blocks in cuts:
        heights = jax.random.uniform(jax.random.fold_in(jax.random.fold_in(own_key, 6), position), (blocks,), jnp.float32, least / len(cuts), largest / len(cuts))
        loudness = loudness * jnp.repeat(jnp.exp(heights), dims[position] // blocks).reshape((-1,) + (1,) * (len(dims) - 1 - position))
    return loudness


def gaussian(stream_key, shape, width, most, shards=(), kind=jnp.bfloat16):
    result = jax.random.normal(stream_key, shape, jnp.float32) * width
    if len(shards) > 0:
        result = level_of(stream_key, shape, shards, -0.22, 0.18) * result
    return jnp.clip(result, min=-most, max=most).astype(kind)


def bell_draw_with(stream_key, extent, spread, reach, cuts, heavy, dtype=jnp.bfloat16):
    result = spread * jax.random.normal(stream_key, extent, jnp.float32)
    if cuts:
        result = result * level_of(stream_key, extent, cuts, -0.22, 0.18)
    return jnp.clip(raised(result, jax.random.fold_in(stream_key, 3), *heavy), -reach, reach).astype(dtype)


def setup_inputs(seed: int = 0, part: int = 0) -> dict:
    seeds = jax.random.split(jax.random.key(seed), 10)
    part_splits = jax.random.split(jax.random.fold_in(seeds[9], part), 10)
    return {
        "one_query": bell_draw_with(part_splits[0], (D_MODEL, Q_DIM), D_MODEL ** -0.5, 0.09375, ((0, 16), (1, 8)), (0, 1, 16, 2.0), jnp.float32),
        "other_query": gaussian(part_splits[1], (D_MODEL, Q_DIM), D_MODEL ** -0.5, 0.0625, ((0, 16), (1, 8)), jnp.float32),
        "one_key": bell_draw_with(part_splits[2], (D_MODEL, KV_DIM), D_MODEL ** -0.5, 0.09375, ((0, 16), (1, 8)), (0, 1, 16, 2.0), jnp.float32),
        "other_key": gaussian(part_splits[3], (D_MODEL, KV_DIM), D_MODEL ** -0.5, 0.0625, ((0, 16), (1, 8)), jnp.float32),
        "one_value": bell_draw_with(part_splits[4], (D_MODEL, KV_DIM), D_MODEL ** -0.5, 0.09375, ((0, 16), (1, 8)), (0, 1, 16, 2.0), jnp.float32),
        "other_value": gaussian(part_splits[5], (D_MODEL, KV_DIM), D_MODEL ** -0.5, 0.0625, ((0, 16), (1, 8)), jnp.float32),
        "mix_share": jnp.clip(0.2 + 0.6 * jax.random.uniform(part_splits[6], (D_MODEL,), jnp.float32) ** level_of(part_splits[6], (D_MODEL,), ((0, 16),), -0.2, 0.2), 0.2, 0.8),
        "norm_train": jnp.clip(1.0 + 0.15 * jax.random.normal(part_splits[7], (D_MODEL,), jnp.float32), 0.25, 1.75),
        "norm_step": jnp.clip(jax.random.uniform(part_splits[8], (D_MODEL,), jnp.float32, -0.3, 0.3) * level_of(part_splits[8], (D_MODEL,), ((0, 128),), -0.4, 0.0), -0.3, 0.3),
    }


def reference(one_query, other_query, one_key, other_key, one_value, other_value, mix_share, norm_train, norm_step):
    whole_query = mix_share[:, None] * one_query + (1.0 - mix_share[:, None]) * other_query
    whole_key = mix_share[:, None] * one_key + (1.0 - mix_share[:, None]) * other_key
    whole_value = mix_share[:, None] * one_value + (1.0 - mix_share[:, None]) * other_value
    scale_query = jnp.max(jnp.abs(whole_query), axis=0)
    serving_query = (whole_query / scale_query).astype(jnp.bfloat16)
    scale_key = jnp.max(jnp.abs(whole_key), axis=0)
    serving_key = (whole_key / scale_key).astype(jnp.bfloat16)
    scale_value = jnp.max(jnp.abs(whole_value), axis=0)
    serving_value = (whole_value / scale_value).astype(jnp.bfloat16)
    serve_norm = (norm_train + norm_step).astype(jnp.bfloat16)
    return serving_query, serving_key, serving_value, scale_query, scale_key, scale_value, serve_norm
```

```python
import jax
import jax.numpy as jnp
from jax import lax
from jax.experimental import pallas as pl
from jax.sharding import PartitionSpec as P

SITE_ROWS = ("site", "rows")
SITE_ROWS_WIDTH = ("site", "rows", "width")
SITE_WIDTH = ("site", "width")


def left_open(*shapes):
    return pl.pallas_call(
        lambda *refs: None,
        out_shape=tuple(jax.ShapeDtypeStruct(s, jnp.bfloat16) for s in shapes),
        out_specs=tuple(pl.BlockSpec(memory_space=pl.ANY) for s in shapes),
    )()


def partner(array):
    n = lax.axis_size("rows")
    return lax.ppermute(array, "rows", [(i, i ^ 1) for i in range(n)])


def onward(array):
    n = lax.axis_size("rows")

    def to(i):
        return (i + 2) % n if i % 2 == 0 else (i - 2) % n

    return lax.ppermute(array, "rows", [(i, to(i)) for i in range(n)])


def body(
    one_query, other_query, one_key, other_key, one_value, other_value, mix_share, norm_train, norm_step):
    n = lax.axis_size("rows")
    wide = lax.axis_size("width")
    me = lax.axis_index("rows")
    core = me & 1
    share = mix_share[:, None]
    rest = 1.0 - share
    wholes = [
        share * one + rest * other
        for one, other in ((one_query, other_query), (one_key, other_key), (one_value, other_value))
    ]
    widths = [a.shape[1] for a in wholes]
    ends = [0, widths[0], widths[0] + widths[1], sum(widths)]
    norm = (norm_train + norm_step).astype(jnp.bfloat16)
    own = jnp.concatenate([jnp.max(jnp.abs(a), axis=0) for a in wholes] + [norm.astype(jnp.float32)])
    seen = lax.all_to_all(
        jnp.broadcast_to(own, (n, own.shape[0])), "rows", split_axis=0, concat_axis=0, tiled=True
    )
    tops = seen.max(axis=0)
    scales = [tops[b:e] for b, e in zip(ends, ends[1:])]
    norms = seen[:, ends[3] :].astype(jnp.bfloat16)

    depth = one_query.shape[0]
    mine = jnp.concatenate([(a / s).astype(jnp.bfloat16) for a, s in zip(wholes, scales)], axis=1)
    outs = left_open(*[(n * depth, w) for w in widths])

    def put(outs, block, owner):
        at = (owner * depth).astype(jnp.int32)
        return [
            lax.dynamic_update_slice(out, block[:, b:e], (at, jnp.int32(0)), allow_negative_indices=False)
            for out, b, e in zip(outs, ends, ends[1:])
        ]

    ahead = 2 - 4 * core

    def chip(hops, of):
        return ((me - core - ahead * hops) & (n - 1)) + of

    own, other = core, core ^ 1
    sibling = partner(mine)
    units = [mine, sibling]
    half = n // 4
    outs = put(outs, mine, me)
    outs = put(outs, sibling, me ^ 1)
    for step in range(1, 2 * half):
        hop, chain = (step + 1) // 2, (step + 1) % 2
        here = onward(units[step - 1])
        units.append(here)
        outs = put(outs, here, chip(hop, core ^ chain))
        across = partner(here)
        outs = put(outs, across, chip(-hop, core ^ 1 ^ chain))

    k = 1
    while k < wide:
        other = lax.ppermute(norms, "width", [(i, i ^ k) for i in range(wide)])
        low = (lax.axis_index("width") & k) == 0
        a, b = jnp.where(low, norms, other), jnp.where(low, other, norms)
        norms = jnp.concatenate([a[:, None], b[:, None]], axis=1).reshape(n, -1)
        k *= 2
    return (*outs, *scales, norms.reshape(-1))


def solution(mesh):
    return jax.shard_map(
        body,
        mesh=mesh,
        in_specs=(P(SITE_ROWS, "width"),) * 6 + (P(SITE_ROWS), P(SITE_ROWS_WIDTH), P(SITE_ROWS_WIDTH)),
        out_specs=(P("site", "width"),) * 3 + (P(SITE_WIDTH),) * 3 + (P("site"),),
        check_vma=False,
    )
```

```python
import jax
import jax.numpy as jnp
from jax import lax
from jax.experimental import pallas as pl
from jax.experimental.pallas import tpu as pltpu
from jax.sharding import PartitionSpec as P

SITE_ROWS = ("site", "rows")
SITE_ROWS_WIDTH = ("site", "rows", "width")
SITE_WIDTH = ("site", "width")
EARLY = (144, 112)
CUTS = (0, 144, 256, 448)
LAST = 128


def spread(row, lane, count):
    rows = lax.broadcasted_iota(jnp.int32, (count, row.shape[1]), 0) + lane
    lanes = lax.broadcasted_iota(jnp.int32, (count, row.shape[1]), 1)
    return jnp.sum(jnp.where(rows == lanes, jnp.broadcast_to(row, rows.shape), 0.0), axis=1, keepdims=True)


def mixed(share, pairs, norm, n):
    depth = share.shape[0]
    widths = [one.shape[1] for one, _ in pairs]
    total = sum(widths)
    arrays = [a for pair in pairs for a in pair]
    gains = [a.reshape(1, -1) for a in norm]
    wide = total + gains[0].shape[1]
    cuts = list(zip(CUTS, CUTS[1:]))
    starts = [0, EARLY[0], sum(EARLY), depth]

    def kernel(*refs):
        share_ref, refs = refs[0], refs[1:]
        array_refs, refs = refs[: len(arrays)], refs[len(arrays) :]
        train_ref, step_ref, *whole_refs, top_ref = refs[:6]
        refs = refs[6:]
        share_buf, array_bufs, gain_bufs = refs[0], refs[1 : 1 + len(arrays)], refs[1 + len(arrays) : 3 + len(arrays)]
        sems, small_sems = refs[-2:]
        small = [
            pltpu.make_async_copy(src, dst, small_sems.at[k])
            for k, (src, dst) in enumerate(
                ((share_ref, share_buf), (train_ref, gain_bufs[0]), (step_ref, gain_bufs[1]))
            )
        ]
        for copy in small:
            copy.start()
        large = []
        for c, (low, high) in enumerate(cuts):
            large.append(
                [
                    pltpu.make_async_copy(src.at[low:high], dst.at[low:high], sems.at[c, k])
                    for k, (src, dst) in enumerate(zip(array_refs, array_bufs))
                ]
            )
            for copy in large[-1]:
                copy.start()
        for copy in small:
            copy.wait()
        gain = (gain_bufs[0][...] + gain_bufs[1][...]).astype(jnp.bfloat16).astype(jnp.float32)
        top_ref[:, :, total:] = jnp.broadcast_to(gain[None], (n, 1, wide - total))
        tops = [None] * len(widths)
        for c, (low, high) in enumerate(cuts):
            column = spread(share_buf[...], low, high - low)
            rest = 1.0 - column
            for copy in large[c]:
                copy.wait()
            at = 0
            for k, w in enumerate(widths):
                whole = column * array_bufs[2 * k][low:high, :] + rest * array_bufs[2 * k + 1][low:high, :]
                piece = max(p for p in range(3) if starts[p] <= low)
                whole_refs[piece][low - starts[piece] : high - starts[piece], at : at + w] = whole
                top = jnp.max(jnp.abs(whole), axis=0, keepdims=True)
                tops[k] = top if c == 0 else jnp.maximum(tops[k], top)
                at += w
        at = 0
        for top, w in zip(tops, widths):
            top_ref[:, :, at : at + w] = jnp.broadcast_to(top[None], (n, 1, w))
            at += w

    inputs = [share.reshape(1, depth), *arrays, *gains]
    return pl.pallas_call(
        kernel,
        in_specs=[pl.BlockSpec(memory_space=pltpu.HBM)] * len(inputs),
        out_specs=[pl.BlockSpec(memory_space=pltpu.VMEM)] * 4,
        out_shape=[jax.ShapeDtypeStruct((b - a, total), jnp.float32) for a, b in zip(starts, starts[1:])]
        + [jax.ShapeDtypeStruct((n, 1, wide), jnp.float32)],
        scratch_shapes=[pltpu.VMEM((1, depth), jnp.float32)]
        + [pltpu.VMEM(a.shape, jnp.float32) for a in arrays]
        + [pltpu.VMEM(g.shape, jnp.float32) for g in gains]
        + [pltpu.SemaphoreType.DMA((len(cuts), len(arrays))), pltpu.SemaphoreType.DMA((3,))],
        compiler_params=pltpu.CompilerParams(vmem_limit_bytes=67043328),
        cost_estimate=pl.CostEstimate(flops=6 * depth * total, bytes_accessed=12 * depth * total, transcendentals=0),
    )(*inputs)


def place(outs, block, hops, flip, skip, depth, shapes):
    n = lax.axis_size("rows")
    ends = [0]
    for shape in shapes:
        ends.append(ends[-1] + shape[1])
    rows = block.shape[0]

    def kernel(*refs):
        block_ref, out_refs, sems = refs[0], refs[-1 - len(shapes) : -1], refs[-1]
        me = lax.axis_index("rows")
        core = me & 1
        owner = ((me - core - (2 - 4 * core) * hops) & (n - 1)) + (core ^ flip)
        at = pl.multiple_of(owner * depth + skip, 32)
        copies = [
            pltpu.make_async_copy(block_ref.at[:, b:e], out.at[pl.ds(at, rows), :], sems.at[k])
            for k, (out, b, e) in enumerate(zip(out_refs, ends, ends[1:]))
        ]
        for copy in copies:
            copy.start()
        for copy in copies:
            copy.wait()

    anywhere = [pl.BlockSpec(memory_space=pltpu.HBM)] * len(shapes)
    given = [] if outs is None else list(outs)
    return pl.pallas_call(
        kernel,
        in_specs=[pl.BlockSpec(memory_space=pltpu.VMEM)] + anywhere[: len(given)],
        out_specs=anywhere,
        out_shape=[jax.ShapeDtypeStruct(shape, jnp.bfloat16) for shape in shapes],
        input_output_aliases={1 + k: k for k in range(len(given))},
        scratch_shapes=[pltpu.SemaphoreType.DMA((len(shapes),))],
        compiler_params=pltpu.CompilerParams(vmem_limit_bytes=4 << 20),
        cost_estimate=pl.CostEstimate(flops=2 * block.size, bytes_accessed=4 * block.size, transcendentals=0),
    )(block, *given)


def partner(array):
    n = lax.axis_size("rows")
    return lax.ppermute(array, "rows", [(i, i ^ 1) for i in range(n)])


def onward(array):
    n = lax.axis_size("rows")

    def to(i):
        return (i + 2) % n if i % 2 == 0 else (i - 2) % n

    return lax.ppermute(array, "rows", [(i, to(i)) for i in range(n)])


def body(one_query, other_query, one_key, other_key, one_value, other_value, mix_share, norm_train, norm_step):
    n = lax.axis_size("rows")
    wide = lax.axis_size("width")
    depth = one_query.shape[0]
    pairs = [(one_query, other_query), (one_key, other_key), (one_value, other_value)]
    widths = [one.shape[1] for one, _ in pairs]
    ends = [0, widths[0], widths[0] + widths[1], sum(widths)]
    *early, late, tops = mixed(mix_share, pairs, (norm_train, norm_step), n)
    coming = [onward(early[0]), onward(early[1])]
    seen = lax.all_to_all(tops, "rows", split_axis=0, concat_axis=0, tiled=True)
    scale = seen.max(axis=(0, 1))
    scales = [scale[b:e] for b, e in zip(ends, ends[1:])]
    scale = scale[: ends[3]]
    norms = seen[:, 0, ends[3] :].astype(jnp.bfloat16)

    def scaled(whole):
        return lax.optimization_barrier((whole / scale).astype(jnp.bfloat16))

    mine_b = scaled(late)
    *early, mine_b, scale = lax.optimization_barrier((*early, mine_b, scale))
    mine = jnp.concatenate([(a / scale).astype(jnp.bfloat16) for a in early] + [mine_b], axis=0)
    shapes = [(n * depth, w) for w in widths]

    def put(outs, block, hops, flip, skip=0):
        return place(outs, block, hops, flip, skip, depth, shapes)

    outs = put(None, mine, 0, 0)
    sibling = partner(mine)
    *coming, scale_in, _ = lax.optimization_barrier((*coming, scale, sibling))
    come = [(a / scale_in).astype(jnp.bfloat16) for a in coming]
    outs = put(outs, sibling, 0, 1)
    units = [mine, sibling]
    steps = n // 2 - 1
    for step in range(1, steps + 1):
        hop, chain = (step + 1) // 2, (step + 1) % 2
        if step == steps:
            cuts = [(step, 0, depth - LAST), (step + 1, depth - LAST, depth)]
        else:
            cuts = [(step, 0, depth)]
        for k, low, high in cuts:
            if k == 1:
                here = onward(mine_b)
                here = jnp.concatenate([*come, here], axis=0)
            else:
                here = onward(units[step - 1][low:high])
            outs = put(outs, here, hop, chain, low)
            across = partner(here)
            outs = put(outs, across, -hop, 1 ^ chain, low)
        units.append(here)

    k, turn = 1, 1
    while k < wide:
        other = lax.ppermute(norms, "width", [(i, i ^ k) for i in range(wide)])
        low = (lax.axis_index("width") & k) == 0
        a, b = jnp.where(low, norms, other), jnp.where(low, other, norms)
        norms = jnp.concatenate([a[:, None], b[:, None]], axis=1).reshape(n, -1)
        k *= 2
        turn += 1
    norms = norms.reshape(-1)
    return (*outs, *scales, norms)


def solution(mesh):
    return jax.shard_map(
        body,
        mesh=mesh,
        in_specs=(P(SITE_ROWS, "width"),) * 6 + (P(SITE_ROWS), P(SITE_ROWS_WIDTH), P(SITE_ROWS_WIDTH)),
        out_specs=(P("site", "width"),) * 3 + (P(SITE_WIDTH),) * 3 + (P("site"),),
        check_vma=False,
    )
```

```python
import jax
import jax.numpy as jnp
from jax import lax
from jax.experimental import pallas as pl
from jax.experimental.pallas import tpu as pltpu
from jax.sharding import PartitionSpec as P

SITE_ROWS = ("site", "rows")
SITE_ROWS_WIDTH = ("site", "rows", "width")
SITE_WIDTH = ("site", "width")
EARLY = (128, 112)
CUTS = (0, 128, 240, 448)
LAST = 96


def spread(row, lane, count):
    rows = lax.broadcasted_iota(jnp.int32, (count, row.shape[1]), 0) + lane
    lanes = lax.broadcasted_iota(jnp.int32, (count, row.shape[1]), 1)
    return jnp.sum(jnp.where(rows == lanes, jnp.broadcast_to(row, rows.shape), 0.0), axis=1, keepdims=True)


def mixed(share, pairs, norm, n):
    depth = share.shape[0]
    widths = [one.shape[1] for one, _ in pairs]
    total = sum(widths)
    arrays = [a for pair in pairs for a in pair]
    gains = [a.reshape(1, -1) for a in norm]
    wide = total + gains[0].shape[1]
    cuts = list(zip(CUTS, CUTS[1:]))
    starts = [0, EARLY[0], sum(EARLY), depth]

    def kernel(*refs):
        share_ref, refs = refs[0], refs[1:]
        array_refs, refs = refs[: len(arrays)], refs[len(arrays) :]
        train_ref, step_ref, *whole_refs, top_ref = refs[:5]
        refs = refs[5:]
        share_buf, array_bufs, gain_bufs = refs[0], refs[1 : 1 + len(arrays)], refs[1 + len(arrays) : 3 + len(arrays)]
        sems, small_sems = refs[-2:]
        small = [
            pltpu.make_async_copy(src, dst, small_sems.at[k])
            for k, (src, dst) in enumerate(
                ((share_ref, share_buf), (train_ref, gain_bufs[0]), (step_ref, gain_bufs[1]))
            )
        ]
        for copy in small:
            copy.start()
        large = []
        for c, (low, high) in enumerate(cuts):
            large.append(
                [
                    pltpu.make_async_copy(src.at[low:high], dst.at[low:high], sems.at[c, k])
                    for k, (src, dst) in enumerate(zip(array_refs, array_bufs))
                ]
            )
            for copy in large[-1]:
                copy.start()
        for copy in small:
            copy.wait()
        gain = (gain_bufs[0][...] + gain_bufs[1][...]).astype(jnp.bfloat16).astype(jnp.float32)
        top_ref[:, :, total:] = jnp.broadcast_to(gain[None], (n, 1, wide - total))
        tops = [None] * len(widths)
        for c, (low, high) in enumerate(cuts):
            column = spread(share_buf[...], low, high - low)
            rest = 1.0 - column
            for copy in large[c]:
                copy.wait()
            at = 0
            for k, w in enumerate(widths):
                whole = column * array_bufs[2 * k][low:high, :] + rest * array_bufs[2 * k + 1][low:high, :]
                piece = max(p for p in range(3) if starts[p] <= low)
                if piece < 2:
                    whole_refs[piece][low - starts[piece] : high - starts[piece], at : at + w] = whole
                top = jnp.max(jnp.abs(whole), axis=0, keepdims=True)
                tops[k] = top if c == 0 else jnp.maximum(tops[k], top)
                at += w
        at = 0
        for top, w in zip(tops, widths):
            top_ref[:, :, at : at + w] = jnp.broadcast_to(top[None], (n, 1, w))
            at += w

    inputs = [share.reshape(1, depth), *arrays, *gains]
    return pl.pallas_call(
        kernel,
        in_specs=[pl.BlockSpec(memory_space=pltpu.HBM)] * len(inputs),
        out_specs=[pl.BlockSpec(memory_space=pltpu.VMEM)] * 3,
        out_shape=[jax.ShapeDtypeStruct((b - a, total), jnp.float32) for a, b in zip(starts, starts[1:3])]
        + [jax.ShapeDtypeStruct((n, 1, wide), jnp.float32)],
        scratch_shapes=[pltpu.VMEM((1, depth), jnp.float32)]
        + [pltpu.VMEM(a.shape, jnp.float32) for a in arrays]
        + [pltpu.VMEM(g.shape, jnp.float32) for g in gains]
        + [pltpu.SemaphoreType.DMA((len(cuts), len(arrays))), pltpu.SemaphoreType.DMA((3,))],
        compiler_params=pltpu.CompilerParams(vmem_limit_bytes=67043328),
        cost_estimate=pl.CostEstimate(flops=6 * depth * total, bytes_accessed=12 * depth * total, transcendentals=0),
    )(*inputs)


def place(outs, blocks, depth, shapes):
    n = lax.axis_size("rows")
    ends = [0]
    for shape in shapes:
        ends.append(ends[-1] + shape[1])

    def kernel(*refs):
        block_refs, out_refs, sems = refs[: len(blocks)], refs[-1 - len(shapes) : -1], refs[-1]
        me = lax.axis_index("rows")
        core = me & 1
        copies = []
        for i, (block_ref, (block, hops, flip, skip)) in enumerate(zip(block_refs, blocks)):
            owner = ((me - core - (2 - 4 * core) * hops) & (n - 1)) + (core ^ flip)
            at = pl.multiple_of(owner * depth + skip, 32)
            for k, (out, b, e) in enumerate(zip(out_refs, ends, ends[1:])):
                to = out.at[pl.ds(at, block.shape[0]), :]
                copies.append(pltpu.make_async_copy(block_ref.at[:, b:e], to, sems.at[i, k]))
                copies[-1].start()
        for copy in copies:
            copy.wait()

    anywhere = [pl.BlockSpec(memory_space=pltpu.HBM)] * len(shapes)
    given = [] if outs is None else list(outs)
    size = sum(block.size for block, *_ in blocks)
    return pl.pallas_call(
        kernel,
        in_specs=[pl.BlockSpec(memory_space=pltpu.VMEM)] * len(blocks) + anywhere[: len(given)],
        out_specs=anywhere,
        out_shape=[jax.ShapeDtypeStruct(shape, jnp.bfloat16) for shape in shapes],
        input_output_aliases={len(blocks) + k: k for k in range(len(given))},
        scratch_shapes=[pltpu.SemaphoreType.DMA((len(blocks), len(shapes)))],
        compiler_params=pltpu.CompilerParams(vmem_limit_bytes=4 << 20),
        cost_estimate=pl.CostEstimate(flops=2 * size, bytes_accessed=4 * size, transcendentals=0),
    )(*[block for block, *_ in blocks], *given)


def partner(array):
    n = lax.axis_size("rows")
    return lax.ppermute(array, "rows", [(i, i ^ 1) for i in range(n)])


def onward(array):
    n = lax.axis_size("rows")

    def to(i):
        return (i + 2) % n if i % 2 == 0 else (i - 2) % n

    return lax.ppermute(array, "rows", [(i, to(i)) for i in range(n)])


def body(one_query, other_query, one_key, other_key, one_value, other_value, mix_share, norm_train, norm_step):
    n = lax.axis_size("rows")
    wide = lax.axis_size("width")
    depth = one_query.shape[0]
    pairs = [(one_query, other_query), (one_key, other_key), (one_value, other_value)]
    widths = [one.shape[1] for one, _ in pairs]
    ends = [0, widths[0], widths[0] + widths[1], sum(widths)]
    *early, tops = mixed(mix_share, pairs, (norm_train, norm_step), n)
    coming = [onward(early[0]), onward(early[1])]
    seen = lax.all_to_all(tops, "rows", split_axis=0, concat_axis=0, tiled=True)
    scale = seen.max(axis=(0, 1))
    scales = [scale[b:e] for b, e in zip(ends, ends[1:])]
    scale = scale[: ends[3]]
    norms = seen[:, 0, ends[3] :].astype(jnp.bfloat16)

    def scaled(whole):
        return lax.optimization_barrier((whole / scale).astype(jnp.bfloat16))

    share = mix_share[sum(EARLY) :, None]
    late = [share * one[sum(EARLY) :] + (1.0 - share) * other[sum(EARLY) :] for one, other in pairs]
    late = lax.optimization_barrier(jnp.concatenate(late, axis=1))
    mine_b = scaled(late)
    *early, mine_b, scale = lax.optimization_barrier((*early, mine_b, scale))
    mine = jnp.concatenate([(a / scale).astype(jnp.bfloat16) for a in early] + [mine_b], axis=0)
    shapes = [(n * depth, w) for w in widths]

    def put(outs, *blocks):
        return place(outs, blocks, depth, shapes)

    outs = put(None, (mine, 0, 0, 0))
    sibling = partner(mine)
    *coming, scale_in, _ = lax.optimization_barrier((*coming, scale, sibling))
    come = [(a / scale_in).astype(jnp.bfloat16) for a in coming]
    outs = put(outs, (sibling, 0, 1, 0))
    units = [mine, sibling]
    steps = n // 2 - 1
    for step in range(1, steps + 1):
        hop, chain = (step + 1) // 2, (step + 1) % 2
        if step == steps:
            cuts = [(step, 0, depth - LAST), (step + 1, depth - LAST, depth)]
        else:
            cuts = [(step, 0, depth)]
        for k, low, high in cuts:
            if k == 1:
                here = onward(mine_b)
                here = jnp.concatenate([*come, here], axis=0)
            else:
                here = onward(units[step - 1][low:high])
            across = partner(here)
            direct, crossed = (here, hop, chain, low), (across, -hop, 1 ^ chain, low)
            if k > steps:
                outs = put(outs, direct, crossed)
            else:
                outs = put(outs, direct)
                outs = put(outs, crossed)
        units.append(here)

    k, turn = 1, 1
    while k < wide:
        other = lax.ppermute(norms, "width", [(i, i ^ k) for i in range(wide)])
        low = (lax.axis_index("width") & k) == 0
        a, b = jnp.where(low, norms, other), jnp.where(low, other, norms)
        norms = jnp.concatenate([a[:, None], b[:, None]], axis=1).reshape(n, -1)
        k *= 2
        turn += 1
    norms = norms.reshape(-1)
    return (*outs, *scales, norms)


def solution(mesh):
    return jax.shard_map(
        body,
        mesh=mesh,
        in_specs=(P(SITE_ROWS, "width"),) * 6 + (P(SITE_ROWS), P(SITE_ROWS_WIDTH), P(SITE_ROWS_WIDTH)),
        out_specs=(P("site", "width"),) * 3 + (P(SITE_WIDTH),) * 3 + (P("site"),),
        check_vma=False,
    )
```
